256 devices in a mesh: pp: 8 (over z_hi, y), cp: 16 (over z_lo, x), tp: 2 (over core).
Axes of the slice: x: 4, y: 4, z: 8 (z_hi: 2, z_lo: 4; z = z_hi * 4 + z_lo), core: 2. Of those that a mesh axis runs over, the one named last changes fastest.
Arguments:
- queries: bfloat16 [8, 2048, 4096], P('pp', 'cp', 'tp'), may hold values from -4.5 to 4.5
- keys: bfloat16 [8, 2048, 256], P('pp', 'cp', 'tp'), may hold values from -4.5 to 4.5
- values: bfloat16 [8, 2048, 256], P('pp', 'cp', 'tp'), may hold values from -6 to 6
- out_weight: bfloat16 [4096, 16384], P('tp', 'cp'), may hold values from -1.5 to 1.5
- span_order: int32 [32], replicated, may hold values from 0 to 31, as said below
Outputs:
- handed: bfloat16 [8, 16, 128, 16384], P('pp', None, 'tp', 'cp')
The draws below stay inside these ranges and needn't reach their ends.
Inputs may be any that keep to these rules, and one draw needn't show every extreme that they name: `span_order`: the two stored blocks 2r and 2r + 1 are the sequence blocks j and 31 - j for some j, in either order; every sequence block appears once.
All inputs are finite; a program needn't handle non-finite values.
Results may differ from the reference program's by a relative error of at most 0.0095.
Values may be sent and summed in bfloat16 or wider, within the bound.
No kernel may reach another device: no remote copies, remote signals or barrier semaphores. Data moves between devices by JAX's collectives and lax.ppermute only.
A program may use at most 128 MiB of HBM per device.

```python
import jax
import jax.numpy as jnp
from jax import lax

D = 16384
HEAD = 128
SPAN = 64
HEADS = 32
KVH = 2
TOKENS = 2048
N_PP = 8
N_CP = 16


def draw_keys(key, part):
    field = jnp.clip(jax.random.normal(jax.random.fold_in(key, 5), (N_PP, TOKENS, KVH * HEAD), jnp.float32), -4.5, 4.5)
    return field.astype(jnp.bfloat16)


def draw_queries(key, part):
    field = jnp.clip(jax.random.normal(jax.random.fold_in(key, 3), (N_PP, TOKENS, HEADS * HEAD), jnp.float32), -4.5, 4.5)
    return field.astype(jnp.bfloat16)


def draw_span_order(key, part):
    picked = jax.random.permutation(jax.random.fold_in(key, 21), N_CP)
    flipped = jax.random.randint(jax.random.fold_in(key, 22), (N_CP,), 0, 2)
    lower = jnp.where(flipped == 1, 2 * N_CP - 1 - picked, picked)
    upper = 2 * N_CP - 1 - lower
    return jnp.stack([lower, upper], axis=1).reshape(-1).astype(jnp.int32)


def block_levels(rng, extent, split, low, top_value):
    level = 1.0
    for axis_at, shards_of in split:
        draws = jax.random.uniform(jax.random.fold_in(jax.random.fold_in(rng, 6), axis_at), (shards_of,), jnp.float32, low / len(split), top_value / len(split))
        level = level * jnp.repeat(jnp.exp(draws), extent[axis_at] // shards_of).reshape((-1,) + (1,) * (len(extent) - 1 - axis_at))
    return level


def centred(stream_key, shape, deviation, reach, cuts=(), held_as=jnp.bfloat16):
    values = deviation * jax.random.normal(stream_key, shape, jnp.float32)
    if cuts:
        values = values * block_levels(stream_key, shape, cuts, -0.22, 0.18)
    return jnp.clip(values, -reach, reach).astype(held_as)


def setup_inputs(seed: int = 0) -> dict:
    key_of = jax.random.split(jax.random.key(seed), 6)
    return {
        "queries": draw_queries(jax.random.fold_in(key_of[5], 71), 0),
        "keys": draw_keys(jax.random.fold_in(key_of[5], 71), 0),
        "values": centred(key_of[2], (N_PP, TOKENS, KVH * HEAD), 1.0, 6.0, ((0, 8), (1, 16), (2, 2))),
        "out_weight": centred(key_of[3], (HEADS * HEAD, D), (max(HEADS * HEAD // 256, 1)) ** -0.5, 1.5, ((0, 2), (1, 16))),
        "span_order": draw_span_order(jax.random.fold_in(key_of[5], 71), 0),
    }


def reference(queries, keys, values, out_weight, span_order):
    offsets = jnp.arange(SPAN, dtype=jnp.int32)
    position = (span_order[:, None] * SPAN + offsets[None, :]).reshape(-1).astype(jnp.int32)
    allowed = position[None, :] <= position[:, None]
    group = HEADS // KVH
    scale = HEAD ** -0.5
    query_heads = queries.reshape(N_PP, TOKENS, HEADS, HEAD)
    key_heads = keys.reshape(N_PP, TOKENS, KVH, HEAD)
    value_heads = values.reshape(N_PP, TOKENS, KVH, HEAD)

    def single(index):
        section = index // HEADS
        head = index % HEADS
        query = query_heads[section, :, head]
        key_rows = key_heads[section, :, head // group]
        value_rows = value_heads[section, :, head // group]
        score = jnp.dot(query, key_rows.T, preferred_element_type=jnp.float32) * scale
        score = jnp.where(allowed, score, -1e30)
        summit = jnp.max(score, axis=-1, keepdims=True)
        weight = jnp.where(allowed, jnp.exp(score - summit), 0.0)
        total = jnp.sum(weight, axis=-1, keepdims=True)
        return jnp.dot(weight.astype(jnp.bfloat16), value_rows, preferred_element_type=jnp.float32) / total

    outputs = lax.map(single, jnp.arange(N_PP * HEADS, dtype=jnp.int32))
    attention = outputs.reshape(N_PP, HEADS, TOKENS, HEAD).transpose(0, 2, 1, 3)
    attention = attention.reshape(N_PP, TOKENS, HEADS * HEAD).astype(jnp.bfloat16)

    def project(section_rows):
        return jnp.dot(section_rows, out_weight, preferred_element_type=jnp.float32).astype(jnp.bfloat16)

    projected = lax.map(project, attention).reshape(N_PP, N_CP, 2 * SPAN, D)
    return jnp.roll(projected, 1, axis=0)
```

```python
import functools

import jax
import jax.numpy as jnp
from jax import lax
from jax.experimental import pallas as pl
from jax.experimental.pallas import tpu as pltpu
from jax.sharding import PartitionSpec as P

HEAD = 128
SIDE = 4
LOG2E = 1.4426950408889634


def flip_of(pp):
    return SIDE - 1 if pp % SIDE == 0 else 0


def section_route(n_pp, k):
    n_cp = SIDE * SIDE
    route = []
    for pp in range(n_pp):
        for z in range(SIDE):
            for x in range(SIDE):
                source = (z ^ flip_of(pp) ^ k) * SIDE + x
                route.append((((pp - 1) % n_pp) * n_cp + source, pp * n_cp + z * SIDE + x))
    return route


def x_route(step):
    return [(z * SIDE + x, z * SIDE + (x + step) % SIDE) for z in range(SIDE) for x in range(SIDE)]


def z_route(k):
    return [((z ^ k) * SIDE + x, z * SIDE + x) for z in range(SIDE) for x in range(SIDE)]


def attention_body(place, order, q, kv0, kv1, kv2, kv3, kv4, out, keys, values, qs, s, peak, mass, acc, *, span, scale):
    heads = q.shape[1] // HEAD
    rows = heads * span
    zr, x, half = place[0], place[1], place[2]
    whole = kv0.shape[0]
    pieces = ((kv0, 0, 0), (kv1, SIDE - 1, 0), (kv2, 1, 0), (kv3, 2, 0), (kv4, 2, whole // 2))
    for ref, offset, first in pieces:
        for at in range(0, ref.shape[0], span):
            block = (first + at) // span
            r = (zr ^ (block // 2)) * SIDE + ((x + offset) & (SIDE - 1))
            to = pl.multiple_of(order[2 * r + block % 2] * span, span)
            keys[pl.ds(to, span), :] = ref[at : at + span, :HEAD]
            values[pl.ds(to, span), :] = ref[at : at + span, HEAD:]
    for h in range(heads):
        qs[h * span : (h + 1) * span, :] = q[:, h * HEAD : (h + 1) * HEAD]
    j = order[2 * (zr * SIDE + x) + half]
    width = 4 * span
    last = j // 4

    def scores(t):
        block = keys[pl.ds(pl.multiple_of(t * width, width), width), :]
        return lax.dot_general(qs[...], block, (((1,), (1,)), ((), ())), preferred_element_type=jnp.float32)

    def keep(t, score):
        s[t] = score
        return jnp.maximum(score[:, :HEAD], score[:, HEAD:])

    row = lax.broadcasted_iota(jnp.int32, (rows, width), 0) & (span - 1)
    col = lax.broadcasted_iota(jnp.int32, (rows, width), 1)
    allowed = col - row <= (j - last * 4) * span
    peak[...] = keep(last, jnp.where(allowed, scores(last), -1e30))

    @pl.loop(0, last)
    def _(t):
        peak[...] = jnp.maximum(peak[...], keep(t, scores(t)))

    factor = scale * LOG2E
    peak[...] = jnp.broadcast_to(jnp.max(peak[...], axis=1, keepdims=True), peak.shape)
    mass[...] = jnp.zeros_like(mass)
    acc[...] = jnp.zeros_like(acc)

    @pl.loop(0, last + 1)
    def _(t):
        top = peak[...]
        low = jnp.exp2((s[t, :, :HEAD] - top) * factor)
        high = jnp.exp2((s[t, :, HEAD:] - top) * factor)
        mass[...] += low + high
        probs = jnp.concatenate([low.astype(jnp.bfloat16), high.astype(jnp.bfloat16)], axis=1)
        block = values[pl.ds(pl.multiple_of(t * width, width), width), :]
        acc[...] += jnp.dot(probs, block, preferred_element_type=jnp.float32)

    total = jnp.sum(mass[...], axis=1, keepdims=True)
    result = (acc[...] / total).astype(jnp.bfloat16)
    for h in range(heads):
        out[:, h * HEAD : (h + 1) * HEAD] = result[h * span : (h + 1) * span, :]


def attend(place, order, q, kv, span):
    heads = q.shape[1] // HEAD
    rows = heads * span
    tokens = order.shape[0] * span
    whole = lambda a: pl.BlockSpec(a.shape, lambda i, place, order: (0, 0))
    return pl.pallas_call(
        functools.partial(attention_body, span=span, scale=HEAD**-0.5),
        out_shape=jax.ShapeDtypeStruct((span, q.shape[1]), jnp.bfloat16),
        grid_spec=pltpu.PrefetchScalarGridSpec(
            num_scalar_prefetch=2,
            grid=(1,),
            in_specs=[pl.BlockSpec((span, q.shape[1]), lambda i, place, order: (place[2], 0))] + [whole(a) for a in kv],
            out_specs=pl.BlockSpec((span, q.shape[1]), lambda i, place, order: (0, 0)),
            scratch_shapes=[
                pltpu.VMEM((tokens, HEAD), jnp.bfloat16),
                pltpu.VMEM((tokens, HEAD), jnp.bfloat16),
                pltpu.VMEM((rows, HEAD), jnp.bfloat16),
                pltpu.VMEM((tokens // (4 * span), rows, 4 * span), jnp.float32),
                pltpu.VMEM((rows, HEAD), jnp.float32),
                pltpu.VMEM((rows, HEAD), jnp.float32),
                pltpu.VMEM((rows, HEAD), jnp.float32),
            ],
        ),
        compiler_params=pltpu.CompilerParams(vmem_limit_bytes=24 << 20),
        cost_estimate=pl.CostEstimate(flops=1 << 30, transcendentals=1 << 20, bytes_accessed=4 << 20),
        name="attend",
    )(place, order, q, *kv)


def project_body(place, a0, a1, a2, a3, a4, w0, w1, *rest, k):
    out, rows, result, sem = rest[-4:]
    span = a0.shape[0]
    at = 0
    for a in (a0, a1, a2, a3, a4):
        rows[at : at + a.shape[0], :] = a[...]
        at += a.shape[0]
    inner = w0.shape[0]
    width = 256
    for n in range(0, w0.shape[1], width):
        value = jnp.dot(rows[:, :inner], w0[:, n : n + width], preferred_element_type=jnp.float32)
        value += jnp.dot(rows[:, inner:], w1[:, n : n + width], preferred_element_type=jnp.float32)
        result[:, n : n + width] = value.astype(jnp.bfloat16)
    copies = []
    for i, offset in enumerate((0, SIDE - 1, 1, 2)):
        r = (place[0] ^ k) * SIDE + ((place[1] + offset) & (SIDE - 1))
        copies.append(pltpu.make_async_copy(result.at[pl.ds(i * span, span), :], out.at[r], sem.at[i]))
    for copy in copies:
        copy.start()
    for copy in copies:
        copy.wait()


def project(place, group, weights, out, k, shape):
    span, width = shape[1], shape[2]
    vmem = pl.BlockSpec(memory_space=pltpu.VMEM)
    operands = [place, *group, *weights] + ([] if out is None else [out])
    return pl.pallas_call(
        functools.partial(project_body, k=k),
        out_shape=jax.ShapeDtypeStruct(shape, jnp.bfloat16),
        in_specs=[pl.BlockSpec(memory_space=pltpu.SMEM)]
        + [vmem] * (len(group) + 2)
        + ([] if out is None else [pl.BlockSpec(memory_space=pl.ANY)]),
        out_specs=pl.BlockSpec(memory_space=pl.ANY),
        scratch_shapes=[
            pltpu.VMEM((SIDE * span, group[0].shape[1]), jnp.bfloat16),
            pltpu.VMEM((SIDE * span, width), jnp.bfloat16),
            pltpu.SemaphoreType.DMA((SIDE,)),
        ],
        input_output_aliases={} if out is None else {len(operands) - 1: 0},
        compiler_params=pltpu.CompilerParams(vmem_limit_bytes=32 << 20),
        cost_estimate=pl.CostEstimate(flops=2 << 30, transcendentals=0, bytes_accessed=12 << 20),
        name=f"project{k}",
    )(*operands)


def over_x(value):
    half = value.shape[0] // 2
    below = lax.ppermute(value, "cp", x_route(1))
    above = lax.ppermute(value, "cp", x_route(-1))
    far_top = lax.ppermute(below[:half], "cp", x_route(1))
    far_bottom = lax.ppermute(above[half:], "cp", x_route(-1))
    return value, below, above, far_top, far_bottom


def on_device(queries, keys, values, out_weight, span_order):
    n_pp = lax.axis_size("pp")
    span = queries.shape[1] // 2
    pp, cp, tp = (lax.axis_index(a) for a in ("pp", "cp", "tp"))
    zr = (cp // SIDE) ^ jnp.where(pp % SIDE == 0, SIDE - 1, 0)
    x = cp % SIDE

    kv = jnp.concatenate([keys[0], values[0]], axis=1)
    slots = [lax.ppermute(kv, ("pp", "cp"), section_route(n_pp, k)) for k in range(SIDE)]
    q = lax.ppermute(queries[0], ("pp", "cp"), section_route(n_pp, 0))
    swap = [(0, 1), (1, 0)]
    weights = (out_weight, lax.ppermute(out_weight, "tp", swap))
    kv_all = over_x(jnp.concatenate(slots, axis=0))

    def place(half):
        return jnp.stack([zr, x, half]).astype(jnp.int32)

    given = attend(place(1 - tp), span_order, q, kv_all, span)
    kept = attend(place(tp), span_order, q, kv_all, span)
    mine = jnp.concatenate([kept, lax.ppermute(given, "tp", swap)], axis=1)

    here = place(tp)
    shape = (lax.axis_size("cp"), span, out_weight.shape[1])
    out = None
    for k in range(SIDE):
        block = mine if k == 0 else lax.ppermute(mine, "cp", z_route(k))
        out = project(here, over_x(block), weights, out, k, shape)
    return out[None]


def solution(mesh):
    placed = (P("pp", "cp", "tp"), P("pp", "cp", "tp"), P("pp", "cp", "tp"), P("tp", "cp"), P())
    return jax.shard_map(
        on_device, mesh=mesh, in_specs=placed, out_specs=P("pp", None, "tp", "cp"), check_vma=False
    )
```

```python
import functools

import jax
import jax.numpy as jnp
from jax import lax
from jax.experimental import pallas as pl
from jax.experimental.pallas import tpu as pltpu
from jax.sharding import PartitionSpec as P


HEAD = 128
SIDE = 4
LOG2E = 1.4426950408889634


def flip_of(pp):
    return SIDE - 1 if pp % SIDE == 0 else 0


def section_route(n_pp):
    route = []
    n_cp = SIDE * SIDE
    for pp in range(n_pp):
        for z in range(SIDE):
            for x in range(SIDE):
                source = (z ^ flip_of(pp)) * SIDE + x
                route.append((((pp - 1) % n_pp) * n_cp + source, pp * n_cp + z * SIDE + x))
    return route


def y_route(n_pp):
    return [(pp, pp - pp % SIDE + (pp + 1) % SIDE) for pp in range(n_pp)]


def gap_route(n_pp):
    n_cp = SIDE * SIDE
    route = []
    for pp in range(0, n_pp, SIDE):
        for z in range(SIDE):
            for x in range(SIDE):
                source = (pp + SIDE) % n_pp * n_cp + (SIDE - 1 - z) * SIDE + x
                route.append((source, pp * n_cp + z * SIDE + x))
    return route


def x_route(step):
    return [(z * SIDE + x, z * SIDE + (x + step) % SIDE) for z in range(SIDE) for x in range(SIDE)]


def z_route(k):
    return [((z ^ k) * SIDE + x, z * SIDE + x) for z in range(SIDE) for x in range(SIDE)]


def attention_body(place, order, qa, qb, kv0, kv1, kv2, kv3, out, keys, values, qs, s, peak, mass, acc, *, span, scale):
    heads = qa.shape[1] // HEAD
    rows = heads * span
    zr, x, half = place[0], place[1], place[2]
    for ref, offset in ((kv0, 0), (kv1, SIDE - 1), (kv2, 1), (kv3, 2)):
        for at in range(0, ref.shape[0], span):
            block = at // span
            r = (zr ^ (block // 2)) * SIDE + ((x + offset) & (SIDE - 1))
            to = pl.multiple_of(order[2 * r + block % 2] * span, span)
            keys[pl.ds(to, span), :] = ref[at : at + span, :HEAD]
            values[pl.ds(to, span), :] = ref[at : at + span, HEAD:]
    for number, q in enumerate((qa, qb)):

        @pl.when(half == number)
        def _(q=q):
            for h in range(heads):
                qs[h * span : (h + 1) * span, :] = q[:, h * HEAD : (h + 1) * HEAD]

    j = order[2 * (zr * SIDE + x) + half]
    width = 4 * span
    last = j // 4

    def scores(t):
        block = keys[pl.ds(pl.multiple_of(t * width, width), width), :]
        return lax.dot_general(qs[...], block, (((1,), (1,)), ((), ())), preferred_element_type=jnp.float32)

    def keep(t, score):
        s[t] = score
        return jnp.maximum(score[:, :HEAD], score[:, HEAD:])

    row = lax.broadcasted_iota(jnp.int32, (rows, width), 0) & (span - 1)
    col = lax.broadcasted_iota(jnp.int32, (rows, width), 1)
    allowed = col - row <= (j - last * 4) * span
    peak[...] = keep(last, jnp.where(allowed, scores(last), -1e30))

    @pl.loop(0, last)
    def _(t):
        peak[...] = jnp.maximum(peak[...], keep(t, scores(t)))

    factor = scale * LOG2E
    peak[...] = jnp.broadcast_to(jnp.max(peak[...], axis=1, keepdims=True), peak.shape)
    mass[...] = jnp.zeros_like(mass)
    acc[...] = jnp.zeros_like(acc)

    @pl.loop(0, last + 1)
    def _(t):
        top = peak[...]
        low = jnp.exp2((s[t, :, :HEAD] - top) * factor)
        high = jnp.exp2((s[t, :, HEAD:] - top) * factor)
        mass[...] += low + high
        probs = jnp.concatenate([low.astype(jnp.bfloat16), high.astype(jnp.bfloat16)], axis=1)
        block = values[pl.ds(pl.multiple_of(t * width, width), width), :]
        acc[...] += jnp.dot(probs, block, preferred_element_type=jnp.float32)

    total = jnp.sum(mass[...], axis=1, keepdims=True)
    result = (acc[...] / total).astype(jnp.bfloat16)
    for h in range(heads):
        out[:, h * HEAD : (h + 1) * HEAD] = result[h * span : (h + 1) * span, :]


def attend(place, order, qs, kv, span):
    inner = qs[0].shape[1]
    rows = inner // HEAD * span
    tokens = order.shape[0] * span
    whole = lambda a: pl.BlockSpec(a.shape, lambda i, place, order: (0, 0))
    return pl.pallas_call(
        functools.partial(attention_body, span=span, scale=HEAD**-0.5),
        out_shape=jax.ShapeDtypeStruct((span, inner), jnp.bfloat16),
        grid_spec=pltpu.PrefetchScalarGridSpec(
            num_scalar_prefetch=2,
            grid=(1,),
            in_specs=[whole(a) for a in (*qs, *kv)],
            out_specs=pl.BlockSpec((span, inner), lambda i, place, order: (0, 0)),
            scratch_shapes=[
                pltpu.VMEM((tokens, HEAD), jnp.bfloat16),
                pltpu.VMEM((tokens, HEAD), jnp.bfloat16),
                pltpu.VMEM((rows, HEAD), jnp.bfloat16),
                pltpu.VMEM((tokens // (4 * span), rows, 4 * span), jnp.float32),
                pltpu.VMEM((rows, HEAD), jnp.float32),
                pltpu.VMEM((rows, HEAD), jnp.float32),
                pltpu.VMEM((rows, HEAD), jnp.float32),
            ],
        ),
        compiler_params=pltpu.CompilerParams(vmem_limit_bytes=16 << 20),
        cost_estimate=pl.CostEstimate(flops=1 << 30, transcendentals=1 << 20, bytes_accessed=4 << 20),
        name="attend",
    )(place, order, *qs, *kv)


def hold_body(source, target, sem):
    copy = pltpu.make_async_copy(source, target, sem)
    copy.start()
    copy.wait()


def hold(array):
    return pl.pallas_call(
        hold_body,
        out_shape=jax.ShapeDtypeStruct(array.shape, array.dtype),
        in_specs=[pl.BlockSpec(memory_space=pl.ANY)],
        out_specs=pl.BlockSpec(memory_space=pltpu.VMEM),
        scratch_shapes=[pltpu.SemaphoreType.DMA],
        compiler_params=pltpu.CompilerParams(vmem_limit_bytes=8 << 20),
        name="hold",
    )(array)


def project_body(place, *refs, k, count, span):
    group, weights, (out, rows, result, sem) = refs[:count], refs[count : count + 2], refs[-4:]
    at = 0
    for ref, first, size in group_pieces(group, k, span):
        rows[at : at + size, :] = ref[first : first + size, :]
        at += size
    width = 256
    for n in range(0, result.shape[1], width):
        value, at = 0.0, 0
        for w in weights:
            inner = w.shape[0]
            value += jnp.dot(rows[:, at : at + inner], w[:, n : n + width], preferred_element_type=jnp.float32)
            at += inner
        result[:, n : n + width] = value.astype(jnp.bfloat16)
    copies = []
    for i, offset in enumerate((0, SIDE - 1, 1, 2)):
        r = (place[0] ^ k) * SIDE + ((place[1] + offset) & (SIDE - 1))
        copies.append(pltpu.make_async_copy(result.at[pl.ds(i * span, span), :], out.at[r], sem.at[i]))
    for copy in copies:
        copy.start()
    for copy in copies:
        copy.wait()


def group_pieces(group, k, span):
    half = span // 2
    if k == 1:
        zt, z1, b1, below, above, c1, far_top, far_bottom = group
        return (
            (zt, 0, half), (z1, 0, half), (b1, 0, half), (below, 0, half), (b1, half, half), (above, 0, half),
            (c1, 0, half), (far_top, 0, half // 2), (far_bottom, 0, half // 2),
        )
    return tuple((a, 0, a.shape[0]) for a in group)


def project(place, group, weights, out, k, shape):
    span, width = shape[1], shape[2]
    vmem = pl.BlockSpec(memory_space=pltpu.VMEM)
    operands = [place, *group, *weights] + ([] if out is None else [out])
    return pl.pallas_call(
        functools.partial(project_body, k=k, count=len(group), span=span),
        out_shape=jax.ShapeDtypeStruct(shape, jnp.bfloat16),
        in_specs=[pl.BlockSpec(memory_space=pltpu.SMEM)]
        + [vmem] * (len(group) + len(weights))
        + ([] if out is None else [pl.BlockSpec(memory_space=pl.ANY)]),
        out_specs=pl.BlockSpec(memory_space=pl.ANY),
        scratch_shapes=[
            pltpu.VMEM((SIDE * span, group[0].shape[1]), jnp.bfloat16),
            pltpu.VMEM((SIDE * span, width), jnp.bfloat16),
            pltpu.SemaphoreType.DMA((SIDE,)),
        ],
        input_output_aliases={} if out is None else {len(operands) - 1: 0},
        compiler_params=pltpu.CompilerParams(vmem_limit_bytes=16 << 20),
        cost_estimate=pl.CostEstimate(flops=2 << 30, transcendentals=0, bytes_accessed=12 << 20),
    )(*operands)


def x_near(value):
    return lax.ppermute(value, "cp", x_route(1)), lax.ppermute(value, "cp", x_route(-1))


def x_far(near):
    below, above = near
    half = below.shape[0] // 2
    return lax.ppermute(below[:half], "cp", x_route(1)), lax.ppermute(above[half:], "cp", x_route(-1))


def section(queries, keys, values, out_weight, span_order):
    n_pp = lax.axis_size("pp")
    span = queries.shape[1] // 2
    pp, cp, tp = (lax.axis_index(a) for a in ("pp", "cp", "tp"))
    zr = (cp // SIDE) ^ jnp.where(pp % SIDE == 0, SIDE - 1, 0)
    x = cp % SIDE
    swap = [(0, 1), (1, 0)]

    kv = jnp.concatenate([keys[0], values[0]], axis=1)
    kv = lax.ppermute(kv, ("pp", "cp"), section_route(n_pp))
    slots = [kv] + [lax.ppermute(kv, "cp", z_route(k)) for k in range(1, SIDE)]
    qa = lax.ppermute(queries[0, :span], ("pp", "cp"), section_route(n_pp))
    qy = lax.ppermute(queries[0, span:], "pp", y_route(n_pp))
    qg = lax.ppermute(qy, ("pp", "cp"), gap_route(n_pp))
    qs = (qa, jnp.where(pp % SIDE == 0, qg, qy))
    weights = lax.ppermute(out_weight, "tp", swap)
    weights = (out_weight, hold(weights))
    kv = jnp.concatenate(slots, axis=0)
    kv_all = (kv, *x_near(kv), lax.ppermute(kv, "cp", x_route(2)))

    def place(half):
        return jnp.stack([zr, x, half]).astype(jnp.int32)

    given = attend(place(1 - tp), span_order, qs, kv_all, span)
    kept = attend(place(tp), span_order, qs, kv_all, span)
    mine = jnp.concatenate([kept, lax.ppermute(given, "tp", swap)], axis=1)

    half = span // 2
    near0 = x_near(mine)
    z2 = lax.ppermute(mine, "cp", z_route(2))
    z1 = lax.ppermute(mine[half:], "cp", z_route(1))
    far0 = x_far(near0)
    zt = lax.ppermute(mine[:half], "cp", z_route(1))
    b1 = lax.ppermute(jnp.concatenate([a[:half] for a in near0], axis=0), "cp", z_route(1))
    near1 = x_near(z1)
    c1 = lax.ppermute(far0[0], "cp", z_route(1))
    far1 = x_far(near1)
    near2 = x_near(z2)
    z3 = lax.ppermute(z2, "cp", z_route(1))
    near3 = x_near(z3)
    far2 = x_far(near2)
    far3 = x_far(near3)

    here = place(tp)
    shape = (lax.axis_size("cp"), span, out_weight.shape[1])
    groups = (
        (0, (mine, *near0, *far0)),
        (1, (zt, z1, b1, *near1, c1, *far1)),
        (2, (z2, *near2, *far2)),
        (3, (z3, *near3, *far3)),
    )
    out = None
    for k, group in groups:
        out = project(here, group, weights, out, k, shape)
    return out[None]


def solution(mesh):
    placed = (P("pp", "cp", "tp"), P("pp", "cp", "tp"), P("pp", "cp", "tp"), P("tp", "cp"), P())
    return jax.shard_map(section, mesh=mesh, in_specs=placed, out_specs=P("pp", None, "tp", "cp"), check_vma=False)
```

```python
import functools

import jax
import jax.numpy as jnp
from jax import lax
from jax.experimental import pallas as pl
from jax.experimental.pallas import tpu as pltpu
from jax.sharding import PartitionSpec as P


HEAD = 128
SIDE = 4
LOG2E = 1.4426950408889634
QUERY_SPLIT = 64


def flip_of(pp):
    return SIDE - 1 if pp % SIDE == 0 else 0


def section_route(n_pp):
    route = []
    n_cp = SIDE * SIDE
    for pp in range(n_pp):
        for z in range(SIDE):
            for x in range(SIDE):
                source = (z ^ flip_of(pp)) * SIDE + x
                route.append((((pp - 1) % n_pp) * n_cp + source, pp * n_cp + z * SIDE + x))
    return route


def y_route(n_pp):
    return [(pp, pp - pp % SIDE + (pp + 1) % SIDE) for pp in range(n_pp)]


def gap_route(n_pp):
    n_cp = SIDE * SIDE
    route = []
    for pp in range(0, n_pp, SIDE):
        for z in range(SIDE):
            for x in range(SIDE):
                source = (pp + SIDE) % n_pp * n_cp + (SIDE - 1 - z) * SIDE + x
                route.append((source, pp * n_cp + z * SIDE + x))
    return route


def x_route(step):
    return [(z * SIDE + x, z * SIDE + (x + step) % SIDE) for z in range(SIDE) for x in range(SIDE)]


def z_route(k):
    return [((z ^ k) * SIDE + x, z * SIDE + x) for z in range(SIDE) for x in range(SIDE)]


def attention_body(place, order, qa, qb, kv0, kv1, kv2, kv3, kept, given, keys, values, qs, s, peak, mass, acc, *, span, scale):
    heads = qa.shape[1] // HEAD
    rows = heads * span
    zr, x, half = place[0], place[1], pl.program_id(0)

    @pl.when(half == 0)
    def _():
        for ref, offset in ((kv0, 0), (kv1, SIDE - 1), (kv2, 1), (kv3, 2)):
            for at in range(0, ref.shape[0], span):
                block = at // span
                r = (zr ^ (block // 2)) * SIDE + ((x + offset) & (SIDE - 1))
                to = pl.multiple_of(order[2 * r + block % 2] * span, span)
                keys[pl.ds(to, span), :] = ref[at : at + span, :HEAD]
                values[pl.ds(to, span), :] = ref[at : at + span, HEAD:]

    more = qa.shape[0] - span
    for number, pieces in enumerate((((qa, 0, span),), ((qa, span, more), (qb, 0, span - more)))):

        @pl.when(half == number)
        def _(pieces=pieces):
            for h in range(heads):
                at = h * span
                for q, first, count in (piece for piece in pieces if piece[2]):
                    qs[at : at + count, :] = q[first : first + count, h * HEAD : (h + 1) * HEAD]
                    at += count

    j = order[2 * (zr * SIDE + x) + half]
    width = 4 * span
    last = j // 4

    def scores(t):
        block = keys[pl.ds(pl.multiple_of(t * width, width), width), :]
        return lax.dot_general(qs[...], block, (((1,), (1,)), ((), ())), preferred_element_type=jnp.float32)

    def keep(t, score):
        s[t] = score
        return jnp.maximum(score[:, :HEAD], score[:, HEAD:])

    row = lax.broadcasted_iota(jnp.int32, (rows, width), 0) & (span - 1)
    col = lax.broadcasted_iota(jnp.int32, (rows, width), 1)
    allowed = col - row <= (j - last * 4) * span
    peak[...] = keep(last, jnp.where(allowed, scores(last), -1e30))

    @pl.loop(0, last)
    def _(t):
        peak[...] = jnp.maximum(peak[...], keep(t, scores(t)))

    factor = scale * LOG2E
    peak[...] = jnp.broadcast_to(jnp.max(peak[...], axis=1, keepdims=True), peak.shape)
    mass[...] = jnp.zeros_like(mass)
    acc[...] = jnp.zeros_like(acc)

    @pl.loop(0, last + 1)
    def _(t):
        top = peak[...]
        low = jnp.exp2((s[t, :, :HEAD] - top) * factor)
        high = jnp.exp2((s[t, :, HEAD:] - top) * factor)
        mass[...] += low + high
        probs = jnp.concatenate([low.astype(jnp.bfloat16), high.astype(jnp.bfloat16)], axis=1)
        block = values[pl.ds(pl.multiple_of(t * width, width), width), :]
        acc[...] += jnp.dot(probs, block, preferred_element_type=jnp.float32)

    total = jnp.sum(mass[...], axis=1, keepdims=True)
    result = (acc[...] / total).astype(jnp.bfloat16)
    for out, wanted in ((kept, half == place[2]), (given, half != place[2])):

        @pl.when(wanted)
        def _(out=out):
            for h in range(heads):
                out[:, h * HEAD : (h + 1) * HEAD] = result[h * span : (h + 1) * span, :]


def attend(place, order, qs, kv, span):
    inner = qs[0].shape[1]
    rows = inner // HEAD * span
    tokens = order.shape[0] * span
    whole = lambda a: pl.BlockSpec(a.shape, lambda i, place, order: (0, 0))
    return pl.pallas_call(
        functools.partial(attention_body, span=span, scale=HEAD**-0.5),
        out_shape=(jax.ShapeDtypeStruct((span, inner), jnp.bfloat16),) * 2,
        grid_spec=pltpu.PrefetchScalarGridSpec(
            num_scalar_prefetch=2,
            grid=(2,),
            in_specs=[whole(a) for a in (*qs, *kv)],
            out_specs=(pl.BlockSpec((span, inner), lambda i, place, order: (0, 0)),) * 2,
            scratch_shapes=[
                pltpu.VMEM((tokens, HEAD), jnp.bfloat16),
                pltpu.VMEM((tokens, HEAD), jnp.bfloat16),
                pltpu.VMEM((rows, HEAD), jnp.bfloat16),
                pltpu.VMEM((tokens // (4 * span), rows, 4 * span), jnp.float32),
                pltpu.VMEM((rows, HEAD), jnp.float32),
                pltpu.VMEM((rows, HEAD), jnp.float32),
                pltpu.VMEM((rows, HEAD), jnp.float32),
            ],
        ),
        compiler_params=pltpu.CompilerParams(vmem_limit_bytes=16 << 20),
        cost_estimate=pl.CostEstimate(flops=1 << 30, transcendentals=1 << 20, bytes_accessed=4 << 20),
        name="attend",
    )(place, order, *qs, *kv)


def hold_body(source, target, sem):
    copy = pltpu.make_async_copy(source, target, sem)
    copy.start()
    copy.wait()


def hold(array):
    return pl.pallas_call(
        hold_body,
        out_shape=jax.ShapeDtypeStruct(array.shape, array.dtype),
        in_specs=[pl.BlockSpec(memory_space=pl.ANY)],
        out_specs=pl.BlockSpec(memory_space=pltpu.VMEM),
        scratch_shapes=[pltpu.SemaphoreType.DMA],
        compiler_params=pltpu.CompilerParams(vmem_limit_bytes=8 << 20),
        name="hold",
    )(array)


def project_body(place, *refs, spots, count):
    arrays, weights, (out, rows, result, sem) = refs[:count], refs[count : count + 2], refs[-4:]
    starts, at = [], 0
    for array, first, size, *_ in spots:
        rows[at : at + size, :] = arrays[array][first : first + size, :]
        starts.append(at)
        at += size
    width = 256
    for n in range(0, result.shape[1], width):
        value, at = 0.0, 0
        for w in weights:
            inner = w.shape[0]
            value += jnp.dot(rows[:, at : at + inner], w[:, n : n + width], preferred_element_type=jnp.float32)
            at += inner
        result[:, n : n + width] = value.astype(jnp.bfloat16)
    copies = []
    for i, (start, (_, _, size, k, offset, row)) in enumerate(zip(starts, spots)):
        r = (place[0] ^ k) * SIDE + ((place[1] + offset) & (SIDE - 1))
        source = result.at[pl.ds(start, size), :]
        copies.append(pltpu.make_async_copy(source, out.at[r, pl.ds(row, size), :], sem.at[i]))
    for copy in copies:
        copy.start()
    for copy in copies:
        copy.wait()


def project(place, pieces, weights, out, shape):
    arrays = []
    for piece in pieces:
        if not any(piece[0] is a for a in arrays):
            arrays.append(piece[0])
    spots = [([piece[0] is a for a in arrays].index(True), *piece[1:]) for piece in pieces]
    count = sum(piece[2] for piece in pieces)
    inner, width = arrays[0].shape[1], shape[2]
    vmem = pl.BlockSpec(memory_space=pltpu.VMEM)
    operands = [place, *arrays, *weights] + ([] if out is None else [out])
    return pl.pallas_call(
        functools.partial(project_body, spots=spots, count=len(arrays)),
        out_shape=jax.ShapeDtypeStruct(shape, jnp.bfloat16),
        in_specs=[pl.BlockSpec(memory_space=pltpu.SMEM)]
        + [vmem] * (len(arrays) + len(weights))
        + ([] if out is None else [pl.BlockSpec(memory_space=pl.ANY)]),
        out_specs=pl.BlockSpec(memory_space=pl.ANY),
        scratch_shapes=[
            pltpu.VMEM((count, inner), jnp.bfloat16),
            pltpu.VMEM((count, width), jnp.bfloat16),
            pltpu.SemaphoreType.DMA((len(spots),)),
        ],
        input_output_aliases={} if out is None else {len(operands) - 1: 0},
        compiler_params=pltpu.CompilerParams(vmem_limit_bytes=16 << 20),
        cost_estimate=pl.CostEstimate(flops=8 * count << 20, transcendentals=0, bytes_accessed=12 << 20),
    )(*operands)


def x_near(value):
    return lax.ppermute(value, "cp", x_route(1)), lax.ppermute(value, "cp", x_route(-1))


def x_far(near):
    below, above = near
    half = below.shape[0] // 2
    return lax.ppermute(below[:half], "cp", x_route(1)), lax.ppermute(above[half:], "cp", x_route(-1))


def section(queries, keys, values, out_weight, span_order):
    n_pp = lax.axis_size("pp")
    span = queries.shape[1] // 2
    pp, cp, tp = (lax.axis_index(a) for a in ("pp", "cp", "tp"))
    zr = (cp // SIDE) ^ jnp.where(pp % SIDE == 0, SIDE - 1, 0)
    x = cp % SIDE
    swap = [(0, 1), (1, 0)]

    kv = jnp.concatenate([keys[0], values[0]], axis=1)
    kv = lax.ppermute(kv, ("pp", "cp"), section_route(n_pp))
    slots = [kv] + [lax.ppermute(kv, "cp", z_route(k)) for k in range(1, SIDE)]
    qa = lax.ppermute(queries[0, :QUERY_SPLIT], ("pp", "cp"), section_route(n_pp))
    qy = lax.ppermute(queries[0, QUERY_SPLIT:], "pp", y_route(n_pp))
    qg = lax.ppermute(qy, ("pp", "cp"), gap_route(n_pp))
    qs = (qa, jnp.where(pp % SIDE == 0, qg, qy))
    weights = lax.ppermute(out_weight, "tp", swap)
    weights = (out_weight, hold(weights))
    kv = jnp.concatenate(slots, axis=0)
    kv_all = (kv, *x_near(kv), lax.ppermute(kv, "cp", x_route(2)))

    here = jnp.stack([zr, x, tp]).astype(jnp.int32)
    kept, given = attend(here, span_order, qs, kv_all, span)
    mine = jnp.concatenate([kept, lax.ppermute(given, "tp", swap)], axis=1)

    half = span // 2
    near0 = x_near(mine)
    z2 = lax.ppermute(mine, "cp", z_route(2))
    z1 = lax.ppermute(mine[half:], "cp", z_route(1))
    far0 = x_far(near0)
    zt = lax.ppermute(mine[:half], "cp", z_route(1))
    near1 = x_near(z1)
    tops = jnp.concatenate([near0[0][:half], near0[1][:half], far0[0]], axis=0)
    b1 = lax.ppermute(tops, "cp", z_route(1))
    far1 = x_far(near1)
    near2 = x_near(z2)
    z3 = lax.ppermute(z2, "cp", z_route(1))
    near3 = x_near(z3)
    far2 = x_far(near2)
    far3 = x_far(near3)

    shape = (lax.axis_size("cp"), span, out_weight.shape[1])
    left, right, far = SIDE - 1, 1, 2

    def near_of(k, pair):
        return [(a, 0, a.shape[0], k, offset, span - a.shape[0]) for a, offset in zip(pair, (left, right))]

    def far_of(k, pair):
        size = pair[0].shape[0]
        return [(pair[0], 0, size, k, far, span - 2 * size), (pair[1], 0, size, k, far, span - size)]

    first = [(mine, 0, span, 0, 0, 0), *near_of(0, near0), *far_of(0, far0)]
    second = [(z2, 0, span, 2, 0, 0), *near_of(2, near2), (z3, 0, span, 3, 0, 0)]
    second += [(zt, 0, half, 1, 0, 0), (z1, 0, half, 1, 0, half), *near_of(1, near1), *far_of(1, far1)]
    third = [*near_of(3, near3), (b1, 0, half, 1, left, 0), (b1, half, half, 1, right, 0), (b1, 2 * half, half, 1, far, 0)]
    fourth = [*far_of(2, far2), *far_of(3, far3)]
    out = None
    for pieces in (first, second, third, fourth):
        out = project(here, pieces, weights, out, shape)
    return out[None]


def solution(mesh):
    placed = (P("pp", "cp", "tp"), P("pp", "cp", "tp"), P("pp", "cp", "tp"), P("tp", "cp"), P())
    return jax.shard_map(section, mesh=mesh, in_specs=placed, out_specs=P("pp", None, "tp", "cp"), check_vma=False)
```

```python
import functools

import jax
import jax.numpy as jnp
from jax import lax
from jax.experimental import pallas as pl
from jax.experimental.pallas import tpu as pltpu
from jax.sharding import PartitionSpec as P


HEAD = 128
SIDE = 4
LOG2E = 1.4426950408889634


SHIFT = SIDE // 2


def flip_of(pp):
    return SHIFT if pp % SIDE == 0 else 0


def section_route(n_pp):
    route = []
    n_cp = SIDE * SIDE
    for pp in range(n_pp):
        for z in range(SIDE):
            for x in range(SIDE):
                source = (z ^ flip_of(pp)) * SIDE + x
                route.append((((pp - 1) % n_pp) * n_cp + source, pp * n_cp + z * SIDE + x))
    return route


def y_route(n_pp):
    return [(pp, pp - pp % SIDE + (pp + 1) % SIDE) for pp in range(n_pp)]


def gap_route(n_pp):
    n_cp = SIDE * SIDE
    route = []
    for pp in range(0, n_pp, SIDE):
        for z in range(SIDE):
            for x in range(SIDE):
                source = (pp + SIDE) % n_pp * n_cp + (z ^ SHIFT) * SIDE + x
                route.append((source, pp * n_cp + z * SIDE + x))
    return route


def x_route(step):
    return [(z * SIDE + x, z * SIDE + (x + step) % SIDE) for z in range(SIDE) for x in range(SIDE)]


def z_route(k):
    return [((z ^ k) * SIDE + x, z * SIDE + x) for z in range(SIDE) for x in range(SIDE)]


def attention_body(place, order, qa, qb, kv0, kv1, kv2, kv3, kept, given, keys, values, qs, s, peak, mass, acc, *, span, scale):
    heads = qa.shape[1] // HEAD
    rows = heads * span
    width = 4 * span
    zr, x = place[0], place[1]
    for ref, offset in ((kv0, 0), (kv1, SIDE - 1), (kv2, 1), (kv3, 2)):
        for at in range(0, ref.shape[0], span):
            block = at // span
            r = (zr ^ (block // 2)) * SIDE + ((x + offset) & (SIDE - 1))
            to = pl.multiple_of(order[2 * r + block % 2] * span, span)
            keys[pl.ds(to, span), :] = ref[at : at + span, :HEAD]
            values[pl.ds(to, span), :] = ref[at : at + span, HEAD:]
    for h in range(heads):
        columns = slice(h * HEAD, (h + 1) * HEAD)
        qs[0, h * span : (h + 1) * span, :] = qa[:, columns]
        qs[1, h * span : (h + 1) * span, :] = qb[:, columns]

    j0, j1 = order[2 * (zr * SIDE + x)], order[2 * (zr * SIDE + x) + 1]
    tiles = j0 // 4 + 1
    steps = s.shape[0]
    unroll = 3
    row = lax.broadcasted_iota(jnp.int32, (span, width), 0)
    col = lax.broadcasted_iota(jnp.int32, (span, width), 1)

    def job(i):
        half = (i >= tiles).astype(jnp.int32)
        t = i - half * tiles
        return half, t, pl.ds(pl.multiple_of(t * width, width), width)

    peak[...] = jnp.full_like(peak, -3e38)

    @pl.loop(0, steps // unroll)
    def _(group):
        for i in range(unroll):
            half, t, tile = job(group * unroll + i)
            allowed = col - row <= (jnp.where(half == 0, j0, j1) - t * 4) * span
            step = rows // 4
            for at in range(0, rows, step):
                part = pl.ds(at, step)
                score = lax.dot_general(
                    qs[half, part, :], keys[tile, :], (((1,), (1,)), ((), ())), preferred_element_type=jnp.float32
                )
                score = (score * (scale * LOG2E)).reshape(step // span, span, width)
                score = jnp.where(allowed[None], score, -1e30).reshape(step, width)
                s[group * unroll + i, part, :] = score
                peak[half, part, :] = jnp.maximum(peak[half, part, :], jnp.maximum(score[:, :HEAD], score[:, HEAD:]))

    for half in range(2):
        peak[half] = jnp.broadcast_to(jnp.max(peak[half], axis=1, keepdims=True), peak.shape[1:])
    mass[...] = jnp.zeros_like(mass)
    acc[...] = jnp.zeros_like(acc)

    @pl.loop(0, steps // unroll)
    def _(group):
        for i in range(unroll):
            half, _, tile = job(group * unroll + i)
            step = rows // 4
            for at in range(0, rows, step):
                part = pl.ds(at, step)
                top = peak[half, part, :]
                low = jnp.exp2(s[group * unroll + i, part, :HEAD] - top)
                high = jnp.exp2(s[group * unroll + i, part, HEAD:] - top)
                mass[half, part, :] += low + high
                probs = jnp.concatenate([low.astype(jnp.bfloat16), high.astype(jnp.bfloat16)], axis=1)
                acc[half, part, :] += jnp.dot(probs, values[tile, :], preferred_element_type=jnp.float32)

    for out, half in ((kept, place[2]), (given, 1 - place[2])):
        total = jnp.sum(mass[half], axis=1, keepdims=True)
        result = (acc[half] / total).astype(jnp.bfloat16)
        for h in range(heads):
            out[:, h * HEAD : (h + 1) * HEAD] = result[h * span : (h + 1) * span, :]


def attend(place, order, qs, kv, span):
    inner = qs[0].shape[1]
    rows = inner // HEAD * span
    tokens = order.shape[0] * span
    whole = lambda a: pl.BlockSpec(a.shape, lambda i, place, order: (0, 0))
    return pl.pallas_call(
        functools.partial(attention_body, span=span, scale=HEAD**-0.5),
        out_shape=(jax.ShapeDtypeStruct((span, inner), jnp.bfloat16),) * 2,
        grid_spec=pltpu.PrefetchScalarGridSpec(
            num_scalar_prefetch=2,
            grid=(1,),
            in_specs=[whole(a) for a in (*qs, *kv)],
            out_specs=(pl.BlockSpec((span, inner), lambda i, place, order: (0, 0)),) * 2,
            scratch_shapes=[
                pltpu.VMEM((tokens, HEAD), jnp.bfloat16),
                pltpu.VMEM((tokens, HEAD), jnp.bfloat16),
                pltpu.VMEM((2, rows, HEAD), jnp.bfloat16),
                pltpu.VMEM((tokens // (4 * span) + 1, rows, 4 * span), jnp.float32),
                pltpu.VMEM((2, rows, HEAD), jnp.float32),
                pltpu.VMEM((2, rows, HEAD), jnp.float32),
                pltpu.VMEM((2, rows, HEAD), jnp.float32),
            ],
        ),
        compiler_params=pltpu.CompilerParams(vmem_limit_bytes=22 << 20),
        cost_estimate=pl.CostEstimate(flops=1 << 30, transcendentals=1 << 20, bytes_accessed=4 << 20),
        name="attend",
    )(place, order, *qs, *kv)


def hold_body(source, target, sem):
    copy = pltpu.make_async_copy(source, target, sem)
    copy.start()
    copy.wait()


def hold(array):
    return pl.pallas_call(
        hold_body,
        out_shape=jax.ShapeDtypeStruct(array.shape, array.dtype),
        in_specs=[pl.BlockSpec(memory_space=pl.ANY)],
        out_specs=pl.BlockSpec(memory_space=pltpu.VMEM),
        scratch_shapes=[pltpu.SemaphoreType.DMA],
        compiler_params=pltpu.CompilerParams(vmem_limit_bytes=8 << 20),
        name="hold",
    )(array)


def project_body(place, *refs, spots, count):
    arrays, weights, (out, rows, result, sem) = refs[:count], refs[count : count + 2], refs[-4:]
    starts, at = [], 0
    for array, first, size, *_ in spots:
        rows[at : at + size, :] = arrays[array][first : first + size, :]
        starts.append(at)
        at += size
    width = 256
    for n in range(0, result.shape[1], width):
        value, at = 0.0, 0
        for w in weights:
            inner = w.shape[0]
            value += jnp.dot(rows[:, at : at + inner], w[:, n : n + width], preferred_element_type=jnp.float32)
            at += inner
        result[:, n : n + width] = value.astype(jnp.bfloat16)
    copies = []
    for i, (start, (_, _, size, k, offset, row)) in enumerate(zip(starts, spots)):
        r = (place[0] ^ k) * SIDE + ((place[1] + offset) & (SIDE - 1))
        source = result.at[pl.ds(start, size), :]
        copies.append(pltpu.make_async_copy(source, out.at[r, pl.ds(row, size), :], sem.at[i]))
    for copy in copies:
        copy.start()
    for copy in copies:
        copy.wait()


def project(place, pieces, weights, out, shape):
    arrays = []
    for piece in pieces:
        if not any(piece[0] is a for a in arrays):
            arrays.append(piece[0])
    spots = [([piece[0] is a for a in arrays].index(True), *piece[1:]) for piece in pieces]
    count = sum(piece[2] for piece in pieces)
    inner, width = arrays[0].shape[1], shape[2]
    vmem = pl.BlockSpec(memory_space=pltpu.VMEM)
    operands = [place, *arrays, *weights] + ([] if out is None else [out])
    return pl.pallas_call(
        functools.partial(project_body, spots=spots, count=len(arrays)),
        out_shape=jax.ShapeDtypeStruct(shape, jnp.bfloat16),
        in_specs=[pl.BlockSpec(memory_space=pltpu.SMEM)]
        + [vmem] * (len(arrays) + len(weights))
        + ([] if out is None else [pl.BlockSpec(memory_space=pl.ANY)]),
        out_specs=pl.BlockSpec(memory_space=pl.ANY),
        scratch_shapes=[
            pltpu.VMEM((count, inner), jnp.bfloat16),
            pltpu.VMEM((count, width), jnp.bfloat16),
            pltpu.SemaphoreType.DMA((len(spots),)),
        ],
        input_output_aliases={} if out is None else {len(operands) - 1: 0},
        compiler_params=pltpu.CompilerParams(vmem_limit_bytes=16 << 20),
        cost_estimate=pl.CostEstimate(flops=8 * count << 20, transcendentals=0, bytes_accessed=12 << 20),
    )(*operands)


def x_near(value):
    return lax.ppermute(value, "cp", x_route(1)), lax.ppermute(value, "cp", x_route(-1))


def x_far(near):
    below, above = near
    half = below.shape[0] // 2
    return lax.ppermute(below[:half], "cp", x_route(1)), lax.ppermute(above[half:], "cp", x_route(-1))


def section(queries, keys, values, out_weight, span_order):
    n_pp = lax.axis_size("pp")
    span = queries.shape[1] // 2
    pp, cp, tp = (lax.axis_index(a) for a in ("pp", "cp", "tp"))
    zr = (cp // SIDE) ^ jnp.where(pp % SIDE == 0, SHIFT, 0)
    x = cp % SIDE
    swap = [(0, 1), (1, 0)]

    kv = jnp.concatenate([keys[0], values[0]], axis=1)
    kv = lax.ppermute(kv, ("pp", "cp"), section_route(n_pp))
    slots = [kv] + [lax.ppermute(kv, "cp", z_route(k)) for k in range(1, SIDE)]
    qa = lax.ppermute(queries[0, :span], ("pp", "cp"), section_route(n_pp))
    qy = lax.ppermute(queries[0, span:], "pp", y_route(n_pp))
    qg = lax.ppermute(qy, ("pp", "cp"), gap_route(n_pp))
    qs = (qa, jnp.where(pp % SIDE == 0, qg, qy))
    weights = lax.ppermute(out_weight, "tp", swap)
    weights = (out_weight, hold(weights))
    kv = jnp.concatenate(slots, axis=0)
    kv_all = (kv, *x_near(kv), lax.ppermute(kv, "cp", x_route(2)))

    here = jnp.stack([zr, x, tp]).astype(jnp.int32)
    kept, given = attend(here, span_order, qs, kv_all, span)
    mine = jnp.concatenate([kept, lax.ppermute(given, "tp", swap)], axis=1)

    half = span // 2
    near0 = x_near(mine)
    z2 = lax.ppermute(mine, "cp", z_route(2))
    z1 = lax.ppermute(mine[half:], "cp", z_route(1))
    far0 = x_far(near0)
    zt = lax.ppermute(mine[:half], "cp", z_route(1))
    near1 = x_near(z1)
    tops = jnp.concatenate([near0[0][:half], near0[1][:half], far0[0]], axis=0)
    b1 = lax.ppermute(tops, "cp", z_route(1))
    far1 = x_far(near1)
    near2 = x_near(z2)
    z3 = lax.ppermute(z2, "cp", z_route(1))
    near3 = x_near(z3)
    far2 = x_far(near2)
    far3 = x_far(near3)

    shape = (lax.axis_size("cp"), span, out_weight.shape[1])
    left, right, far = SIDE - 1, 1, 2

    def near_of(k, pair):
        return [(a, 0, a.shape[0], k, offset, span - a.shape[0]) for a, offset in zip(pair, (left, right))]

    def far_of(k, pair):
        size = pair[0].shape[0]
        return [(pair[0], 0, size, k, far, span - 2 * size), (pair[1], 0, size, k, far, span - size)]

    first = [(mine, 0, span, 0, 0, 0), *near_of(0, near0), *far_of(0, far0)]
    second = [(z2, 0, span, 2, 0, 0), *near_of(2, near2), (z3, 0, span, 3, 0, 0)]
    second += [(zt, 0, half, 1, 0, 0), (z1, 0, half, 1, 0, half), *near_of(1, near1), *far_of(1, far1)]
    third = [*near_of(3, near3), (b1, 0, half, 1, left, 0), (b1, half, half, 1, right, 0), (b1, 2 * half, half, 1, far, 0)]
    fourth = [*far_of(2, far2), *far_of(3, far3)]
    out = None
    for pieces in (first, second, third, fourth):
        out = project(here, pieces, weights, out, shape)
    return out[None]


def solution(mesh):
    placed = (P("pp", "cp", "tp"), P("pp", "cp", "tp"), P("pp", "cp", "tp"), P("tp", "cp"), P())
    return jax.shard_map(section, mesh=mesh, in_specs=placed, out_specs=P("pp", None, "tp", "cp"), check_vma=False)
```

```python
import functools

import jax
import jax.numpy as jnp
from jax import lax
from jax.experimental import pallas as pl
from jax.experimental.pallas import tpu as pltpu
from jax.sharding import PartitionSpec as P


HEAD = 128
SIDE = 4
LOG2E = 1.4426950408889634
BUNDLED = 40


SHIFT = SIDE // 2


def flip_of(pp):
    return SHIFT if pp % SIDE == 0 else 0


def section_route(n_pp):
    route = []
    n_cp = SIDE * SIDE
    for pp in range(n_pp):
        for z in range(SIDE):
            for x in range(SIDE):
                source = (z ^ flip_of(pp)) * SIDE + x
                route.append((((pp - 1) % n_pp) * n_cp + source, pp * n_cp + z * SIDE + x))
    return route


def y_route(n_pp):
    return [(pp, pp - pp % SIDE + (pp + 1) % SIDE) for pp in range(n_pp)]


def gap_route(n_pp):
    n_cp = SIDE * SIDE
    route = []
    for pp in range(0, n_pp, SIDE):
        for z in range(SIDE):
            for x in range(SIDE):
                source = (pp + SIDE) % n_pp * n_cp + (z ^ SHIFT) * SIDE + x
                route.append((source, pp * n_cp + z * SIDE + x))
    return route


def x_route(step):
    return [(z * SIDE + x, z * SIDE + (x + step) % SIDE) for z in range(SIDE) for x in range(SIDE)]


def z_route(k):
    return [((z ^ k) * SIDE + x, z * SIDE + x) for z in range(SIDE) for x in range(SIDE)]


def attention_body(place, order, qa, qb, kv0, kv1, kv2, kv3, kept, given, keys, values, qs, s, peak, mass, acc, *, span, scale):
    heads = qa.shape[1] // HEAD
    rows = heads * span
    width = 4 * span
    zr, x = place[0], place[1]
    for ref, offset in ((kv0, 0), (kv1, SIDE - 1), (kv2, 1), (kv3, 2)):
        for at in range(0, ref.shape[0], span):
            block = at // span
            r = (zr ^ (block // 2)) * SIDE + ((x + offset) & (SIDE - 1))
            to = pl.multiple_of(order[2 * r + block % 2] * span, span)
            keys[pl.ds(to, span), :] = ref[at : at + span, :HEAD]
            values[pl.ds(to, span), :] = ref[at : at + span, HEAD:]
    for h in range(heads):
        columns = slice(h * HEAD, (h + 1) * HEAD)
        qs[0, h * span : (h + 1) * span, :] = qa[:, columns]
        qs[1, h * span : (h + 1) * span, :] = qb[:, columns]

    j0, j1 = order[2 * (zr * SIDE + x)], order[2 * (zr * SIDE + x) + 1]
    tiles = j0 // 4 + 1
    steps = s.shape[0]
    unroll = 3
    row = lax.broadcasted_iota(jnp.int32, (span, width), 0)
    col = lax.broadcasted_iota(jnp.int32, (span, width), 1)

    def job(i):
        half = (i >= tiles).astype(jnp.int32)
        t = i - half * tiles
        return half, t, pl.ds(pl.multiple_of(t * width, width), width)

    peak[...] = jnp.full_like(peak, -3e38)

    @pl.loop(0, steps // unroll)
    def _(group):
        for i in range(unroll):
            half, t, tile = job(group * unroll + i)
            allowed = col - row <= (jnp.where(half == 0, j0, j1) - t * 4) * span
            step = rows // 2
            for at in range(0, rows, step):
                part = pl.ds(at, step)
                score = lax.dot_general(
                    qs[half, part, :], keys[tile, :], (((1,), (1,)), ((), ())), preferred_element_type=jnp.float32
                )
                score = (score * (scale * LOG2E)).reshape(step // span, span, width)
                score = jnp.where(allowed[None], score, -1e30).reshape(step, width)
                s[group * unroll + i, part, :] = score
                peak[half, part, :] = jnp.maximum(peak[half, part, :], jnp.maximum(score[:, :HEAD], score[:, HEAD:]))

    mass[...] = jnp.zeros_like(mass)
    acc[...] = jnp.zeros_like(acc)
    for half in range(2):
        peak[half] = jnp.broadcast_to(jnp.max(peak[half], axis=1, keepdims=True), peak.shape[1:])

    @pl.loop(0, steps // unroll)
    def _(group):
        for i in range(unroll):
            half, _, tile = job(group * unroll + i)
            step = rows // 2
            for at in range(0, rows, step):
                part = pl.ds(at, step)
                top = peak[half, part, :]
                low = jnp.exp2(s[group * unroll + i, part, :HEAD] - top)
                high = jnp.exp2(s[group * unroll + i, part, HEAD:] - top)
                mass[half, part, :] += low + high
                probs = jnp.concatenate([low.astype(jnp.bfloat16), high.astype(jnp.bfloat16)], axis=1)
                acc[half, part, :] += jnp.dot(probs, values[tile, :], preferred_element_type=jnp.float32)

    for out, half in ((kept, place[2]), (given, 1 - place[2])):
        total = jnp.sum(mass[half], axis=1, keepdims=True)
        result = (acc[half] / total).astype(jnp.bfloat16)
        for h in range(heads):
            out[:, h * HEAD : (h + 1) * HEAD] = result[h * span : (h + 1) * span, :]


def attend(place, order, qs, kv, span):
    inner = qs[0].shape[1]
    rows = inner // HEAD * span
    tokens = order.shape[0] * span
    whole = lambda a: pl.BlockSpec(a.shape, lambda i, place, order: (0, 0))
    return pl.pallas_call(
        functools.partial(attention_body, span=span, scale=HEAD**-0.5),
        out_shape=(jax.ShapeDtypeStruct((span, inner), jnp.bfloat16),) * 2,
        grid_spec=pltpu.PrefetchScalarGridSpec(
            num_scalar_prefetch=2,
            grid=(1,),
            in_specs=[whole(a) for a in (*qs, *kv)],
            out_specs=(pl.BlockSpec((span, inner), lambda i, place, order: (0, 0)),) * 2,
            scratch_shapes=[
                pltpu.VMEM((tokens, HEAD), jnp.bfloat16),
                pltpu.VMEM((tokens, HEAD), jnp.bfloat16),
                pltpu.VMEM((2, rows, HEAD), jnp.bfloat16),
                pltpu.VMEM((tokens // (4 * span) + 1, rows, 4 * span), jnp.float32),
                pltpu.VMEM((2, rows, HEAD), jnp.float32),
                pltpu.VMEM((2, rows, HEAD), jnp.float32),
                pltpu.VMEM((2, rows, HEAD), jnp.float32),
            ],
        ),
        compiler_params=pltpu.CompilerParams(vmem_limit_bytes=22 << 20),
        cost_estimate=pl.CostEstimate(flops=1 << 30, transcendentals=1 << 20, bytes_accessed=4 << 20),
        name="attend",
    )(place, order, *qs, *kv)


def hold_body(source, target, sem):
    copy = pltpu.make_async_copy(source, target, sem)
    copy.start()
    copy.wait()


def hold(array):
    return pl.pallas_call(
        hold_body,
        out_shape=jax.ShapeDtypeStruct(array.shape, array.dtype),
        in_specs=[pl.BlockSpec(memory_space=pl.ANY)],
        out_specs=pl.BlockSpec(memory_space=pltpu.VMEM),
        scratch_shapes=[pltpu.SemaphoreType.DMA],
        compiler_params=pltpu.CompilerParams(vmem_limit_bytes=8 << 20),
        name="hold",
    )(array)


def project_body(place, *refs, spots, count):
    arrays, weights, (out, rows, result, sem) = refs[:count], refs[count : count + 2], refs[-4:]
    starts, at = [], 0
    for array, first, size, *_ in spots:
        rows[at : at + size, :] = arrays[array][first : first + size, :]
        starts.append(at)
        at += size
    width = 256
    for n in range(0, result.shape[1], width):
        value, at = 0.0, 0
        for w in weights:
            inner = w.shape[0]
            value += jnp.dot(rows[:, at : at + inner], w[:, n : n + width], preferred_element_type=jnp.float32)
            at += inner
        result[:, n : n + width] = value.astype(jnp.bfloat16)
    copies = []
    for i, (start, (_, _, size, k, offset, row)) in enumerate(zip(starts, spots)):
        r = (place[0] ^ k) * SIDE + ((place[1] + offset) & (SIDE - 1))
        source = result.at[pl.ds(start, size), :]
        copies.append(pltpu.make_async_copy(source, out.at[r, pl.ds(row, size), :], sem.at[i]))
    for copy in copies:
        copy.start()
    for copy in copies:
        copy.wait()


def project(place, pieces, weights, out, shape):
    arrays = []
    for piece in pieces:
        if not any(piece[0] is a for a in arrays):
            arrays.append(piece[0])
    spots = [([piece[0] is a for a in arrays].index(True), *piece[1:]) for piece in pieces]
    count = sum(piece[2] for piece in pieces)
    inner, width = arrays[0].shape[1], shape[2]
    vmem = pl.BlockSpec(memory_space=pltpu.VMEM)
    operands = [place, *arrays, *weights] + ([] if out is None else [out])
    return pl.pallas_call(
        functools.partial(project_body, spots=spots, count=len(arrays)),
        out_shape=jax.ShapeDtypeStruct(shape, jnp.bfloat16),
        in_specs=[pl.BlockSpec(memory_space=pltpu.SMEM)]
        + [vmem] * (len(arrays) + len(weights))
        + ([] if out is None else [pl.BlockSpec(memory_space=pl.ANY)]),
        out_specs=pl.BlockSpec(memory_space=pl.ANY),
        scratch_shapes=[
            pltpu.VMEM((count, inner), jnp.bfloat16),
            pltpu.VMEM((count, width), jnp.bfloat16),
            pltpu.SemaphoreType.DMA((len(spots),)),
        ],
        input_output_aliases={} if out is None else {len(operands) - 1: 0},
        compiler_params=pltpu.CompilerParams(vmem_limit_bytes=16 << 20),
        cost_estimate=pl.CostEstimate(flops=8 * count << 20, transcendentals=0, bytes_accessed=12 << 20),
    )(*operands)


def x_near(value):
    return lax.ppermute(value, "cp", x_route(1)), lax.ppermute(value, "cp", x_route(-1))


def x_far(near):
    below, above = near
    half = (below.shape[0] // 2 + 15) // 16 * 16
    return lax.ppermute(below[:half], "cp", x_route(1)), lax.ppermute(above[half:], "cp", x_route(-1))


def section(queries, keys, values, out_weight, span_order):
    n_pp = lax.axis_size("pp")
    span = queries.shape[1] // 2
    pp, cp, tp = (lax.axis_index(a) for a in ("pp", "cp", "tp"))
    zr = (cp // SIDE) ^ jnp.where(pp % SIDE == 0, SHIFT, 0)
    x = cp % SIDE
    swap = [(0, 1), (1, 0)]

    kv = jnp.concatenate([keys[0], values[0]], axis=1)
    kv = lax.ppermute(kv, ("pp", "cp"), section_route(n_pp))
    slots = [kv] + [lax.ppermute(kv, "cp", z_route(k)) for k in range(1, SIDE)]
    qa = lax.ppermute(queries[0, :span], ("pp", "cp"), section_route(n_pp))
    qy = lax.ppermute(queries[0, span:], "pp", y_route(n_pp))
    qg = lax.ppermute(qy, ("pp", "cp"), gap_route(n_pp))
    qs = (qa, jnp.where(pp % SIDE == 0, qg, qy))
    weights = lax.ppermute(out_weight, "tp", swap)
    weights = (out_weight, hold(weights))
    kv = jnp.concatenate(slots, axis=0)
    kv_all = (kv, *x_near(kv), lax.ppermute(kv, "cp", x_route(2)))

    here = jnp.stack([zr, x, tp]).astype(jnp.int32)
    kept, given = attend(here, span_order, qs, kv_all, span)
    mine = jnp.concatenate([kept, lax.ppermute(given, "tp", swap)], axis=1)

    half = span // 2
    near0 = x_near(mine)
    z2 = lax.ppermute(mine, "cp", z_route(2))
    z1 = lax.ppermute(mine[BUNDLED:], "cp", z_route(1))
    far0 = x_far(near0)
    zt = lax.ppermute(mine[:BUNDLED], "cp", z_route(1))
    near1 = x_near(z1)
    tops = jnp.concatenate([near0[0][:BUNDLED], near0[1][:BUNDLED], far0[0], far0[1][: BUNDLED - half]], axis=0)
    b1 = lax.ppermute(tops, "cp", z_route(1))
    far1 = x_far(near1)
    near2 = x_near(z2)
    z3 = lax.ppermute(z2, "cp", z_route(1))
    near3 = x_near(z3)
    far2 = x_far(near2)
    far3 = x_far(near3)

    shape = (lax.axis_size("cp"), span, out_weight.shape[1])
    left, right, far = SIDE - 1, 1, 2

    def near_of(k, pair):
        return [(a, 0, a.shape[0], k, offset, span - a.shape[0]) for a, offset in zip(pair, (left, right))]

    def far_of(k, pair):
        top, bottom = (a.shape[0] for a in pair)
        return [(pair[0], 0, top, k, far, span - top - bottom), (pair[1], 0, bottom, k, far, span - bottom)]

    first = [(mine, 0, span, 0, 0, 0), *near_of(0, near0), *far_of(0, far0)]
    second = [(z2, 0, span, 2, 0, 0), *near_of(2, near2), (z3, 0, span, 3, 0, 0)]
    second += [(zt, 0, BUNDLED, 1, 0, 0), (z1, 0, span - BUNDLED, 1, 0, BUNDLED)]
    second += [*near_of(1, near1), *far_of(1, far1)]
    third = near_of(3, near3)
    third += [(b1, i * BUNDLED, BUNDLED, 1, offset, 0) for i, offset in enumerate((left, right, far))]
    fourth = [*far_of(2, far2), *far_of(3, far3)]
    out = None
    for pieces in (first, second, third, fourth):
        out = project(here, pieces, weights, out, shape)
    return out[None]


def solution(mesh):
    placed = (P("pp", "cp", "tp"), P("pp", "cp", "tp"), P("pp", "cp", "tp"), P("tp", "cp"), P())
    return jax.shard_map(section, mesh=mesh, in_specs=placed, out_specs=P("pp", None, "tp", "cp"), check_vma=False)
```

```python
import functools

import jax
import jax.numpy as jnp
from jax import lax
from jax.experimental import pallas as pl
from jax.experimental.pallas import tpu as pltpu
from jax.sharding import PartitionSpec as P


HEAD = 128
SIDE = 4
LOG2E = 1.4426950408889634
BUNDLED = 40


SHIFT = SIDE // 2


def flip_of(pp):
    return SHIFT if pp % SIDE == 0 else 0


def section_route(n_pp):
    route = []
    n_cp = SIDE * SIDE
    for pp in range(n_pp):
        for z in range(SIDE):
            for x in range(SIDE):
                source = (z ^ flip_of(pp)) * SIDE + x
                route.append((((pp - 1) % n_pp) * n_cp + source, pp * n_cp + z * SIDE + x))
    return route


def y_route(n_pp):
    return [(pp, pp - pp % SIDE + (pp + 1) % SIDE) for pp in range(n_pp)]


def gap_route(n_pp):
    n_cp = SIDE * SIDE
    route = []
    for pp in range(0, n_pp, SIDE):
        for z in range(SIDE):
            for x in range(SIDE):
                source = (pp + SIDE) % n_pp * n_cp + (z ^ SHIFT) * SIDE + x
                route.append((source, pp * n_cp + z * SIDE + x))
    return route


def x_route(step):
    return [(z * SIDE + x, z * SIDE + (x + step) % SIDE) for z in range(SIDE) for x in range(SIDE)]


def z_route(k):
    return [((z ^ k) * SIDE + x, z * SIDE + x) for z in range(SIDE) for x in range(SIDE)]


def attention_body(place, order, qa, qb, kv0, kv1, kv2, kv3, kept, given, keys, values, qs, s, peak, mass, acc, *, span, scale):
    heads = qa.shape[1] // HEAD
    rows = heads * span
    width = 4 * span
    zr, x = place[0], place[1]
    for ref, offset in ((kv0, 0), (kv1, SIDE - 1), (kv2, 1), (kv3, 2)):
        for at in range(0, ref.shape[0], span):
            block = at // span
            r = (zr ^ (block // 2)) * SIDE + ((x + offset) & (SIDE - 1))
            to = pl.multiple_of(order[2 * r + block % 2] * span, span)
            keys[pl.ds(to, span), :] = ref[at : at + span, :HEAD]
            values[pl.ds(to, span), :] = ref[at : at + span, HEAD:]
    for h in range(heads):
        columns = slice(h * HEAD, (h + 1) * HEAD)
        qs[0, h * span : (h + 1) * span, :] = qa[:, columns]
        qs[1, h * span : (h + 1) * span, :] = qb[:, columns]

    j0, j1 = order[2 * (zr * SIDE + x)], order[2 * (zr * SIDE + x) + 1]
    tiles = j0 // 4 + 1
    steps = s.shape[0]
    unroll = 3
    row = lax.broadcasted_iota(jnp.int32, (span, width), 0)
    col = lax.broadcasted_iota(jnp.int32, (span, width), 1)

    def job(i):
        half = (i >= tiles).astype(jnp.int32)
        t = i - half * tiles
        return half, t, pl.ds(pl.multiple_of(t * width, width), width)

    peak[...] = jnp.full_like(peak, -3e38)

    @pl.loop(0, steps // unroll)
    def _(group):
        for i in range(unroll):
            half, t, tile = job(group * unroll + i)
            allowed = col - row <= (jnp.where(half == 0, j0, j1) - t * 4) * span
            step = rows // 2
            for at in range(0, rows, step):
                part = pl.ds(at, step)
                score = lax.dot_general(
                    qs[half, part, :], keys[tile, :], (((1,), (1,)), ((), ())), preferred_element_type=jnp.float32
                )
                score = (score * (scale * LOG2E)).reshape(step // span, span, width)
                score = jnp.where(allowed[None], score, -1e30).reshape(step, width)
                s[group * unroll + i, part, :] = score
                peak[half, part, :] = jnp.maximum(peak[half, part, :], jnp.maximum(score[:, :HEAD], score[:, HEAD:]))

    mass[...] = jnp.zeros_like(mass)
    acc[...] = jnp.zeros_like(acc)
    for half in range(2):
        peak[half] = jnp.broadcast_to(jnp.max(peak[half], axis=1, keepdims=True), peak.shape[1:])

    @pl.loop(0, steps // unroll)
    def _(group):
        for i in range(unroll):
            half, _, tile = job(group * unroll + i)
            step = rows // 2
            for at in range(0, rows, step):
                part = pl.ds(at, step)
                top = peak[half, part, :]
                low = jnp.exp2(s[group * unroll + i, part, :HEAD] - top)
                high = jnp.exp2(s[group * unroll + i, part, HEAD:] - top)
                mass[half, part, :] += low + high
                probs = jnp.concatenate([low.astype(jnp.bfloat16), high.astype(jnp.bfloat16)], axis=1)
                acc[half, part, :] += jnp.dot(probs, values[tile, :], preferred_element_type=jnp.float32)

    for out, half in ((kept, place[2]), (given, 1 - place[2])):
        total = jnp.sum(mass[half], axis=1, keepdims=True)
        result = (acc[half] / total).astype(jnp.bfloat16)
        for h in range(heads):
            out[:, h * HEAD : (h + 1) * HEAD] = result[h * span : (h + 1) * span, :]


def attend(place, order, qs, kv, span):
    inner = qs[0].shape[1]
    rows = inner // HEAD * span
    tokens = order.shape[0] * span
    whole = lambda a: pl.BlockSpec(a.shape, lambda i, place, order: (0, 0))
    return pl.pallas_call(
        functools.partial(attention_body, span=span, scale=HEAD**-0.5),
        out_shape=(jax.ShapeDtypeStruct((span, inner), jnp.bfloat16),) * 2,
        grid_spec=pltpu.PrefetchScalarGridSpec(
            num_scalar_prefetch=2,
            grid=(1,),
            in_specs=[whole(a) for a in (*qs, *kv)],
            out_specs=(pl.BlockSpec((span, inner), lambda i, place, order: (0, 0)),) * 2,
            scratch_shapes=[
                pltpu.VMEM((tokens, HEAD), jnp.bfloat16),
                pltpu.VMEM((tokens, HEAD), jnp.bfloat16),
                pltpu.VMEM((2, rows, HEAD), jnp.bfloat16),
                pltpu.VMEM((tokens // (4 * span) + 1, rows, 4 * span), jnp.float32),
                pltpu.VMEM((2, rows, HEAD), jnp.float32),
                pltpu.VMEM((2, rows, HEAD), jnp.float32),
                pltpu.VMEM((2, rows, HEAD), jnp.float32),
            ],
        ),
        compiler_params=pltpu.CompilerParams(vmem_limit_bytes=22 << 20),
        cost_estimate=pl.CostEstimate(flops=1 << 30, transcendentals=1 << 20, bytes_accessed=4 << 20),
        name="attend",
    )(place, order, *qs, *kv)


def hold_body(source, target, sem):
    copy = pltpu.make_async_copy(source, target, sem)
    copy.start()
    copy.wait()


def hold(array):
    return pl.pallas_call(
        hold_body,
        out_shape=jax.ShapeDtypeStruct(array.shape, array.dtype),
        in_specs=[pl.BlockSpec(memory_space=pl.ANY)],
        out_specs=pl.BlockSpec(memory_space=pltpu.VMEM),
        scratch_shapes=[pltpu.SemaphoreType.DMA],
        compiler_params=pltpu.CompilerParams(vmem_limit_bytes=8 << 20),
        name="hold",
    )(array)


def project_body(place, *refs, spots, count):
    arrays, weights, (out, rows, result, sem) = refs[:count], refs[count : count + 2], refs[-4:]
    starts, at = [], 0
    for array, first, size, *_ in spots:
        rows[at : at + size, :] = arrays[array][first : first + size, :]
        starts.append(at)
        at += size
    width = 256
    for n in range(0, result.shape[1], width):
        value, at = 0.0, 0
        for w in weights:
            inner = w.shape[0]
            value += jnp.dot(rows[:, at : at + inner], w[:, n : n + width], preferred_element_type=jnp.float32)
            at += inner
        result[:, n : n + width] = value.astype(jnp.bfloat16)
    copies = []
    for i, (start, (_, _, size, k, offset, row)) in enumerate(zip(starts, spots)):
        r = (place[0] ^ k) * SIDE + ((place[1] + offset) & (SIDE - 1))
        source = result.at[pl.ds(start, size), :]
        copies.append(pltpu.make_async_copy(source, out.at[r, pl.ds(row, size), :], sem.at[i]))
    for copy in copies:
        copy.start()
    for copy in copies:
        copy.wait()


def project(place, pieces, weights, out, shape):
    arrays = []
    for piece in pieces:
        if not any(piece[0] is a for a in arrays):
            arrays.append(piece[0])
    spots = [([piece[0] is a for a in arrays].index(True), *piece[1:]) for piece in pieces]
    count = sum(piece[2] for piece in pieces)
    inner, width = arrays[0].shape[1], shape[2]
    vmem = pl.BlockSpec(memory_space=pltpu.VMEM)
    operands = [place, *arrays, *weights] + ([] if out is None else [out])
    return pl.pallas_call(
        functools.partial(project_body, spots=spots, count=len(arrays)),
        out_shape=jax.ShapeDtypeStruct(shape, jnp.bfloat16),
        in_specs=[pl.BlockSpec(memory_space=pltpu.SMEM)]
        + [vmem] * (len(arrays) + len(weights))
        + ([] if out is None else [pl.BlockSpec(memory_space=pl.ANY)]),
        out_specs=pl.BlockSpec(memory_space=pl.ANY),
        scratch_shapes=[
            pltpu.VMEM((count, inner), jnp.bfloat16),
            pltpu.VMEM((count, width), jnp.bfloat16),
            pltpu.SemaphoreType.DMA((len(spots),)),
        ],
        input_output_aliases={} if out is None else {len(operands) - 1: 0},
        compiler_params=pltpu.CompilerParams(vmem_limit_bytes=16 << 20),
        cost_estimate=pl.CostEstimate(flops=8 * count << 20, transcendentals=0, bytes_accessed=12 << 20),
    )(*operands)


def x_near(value):
    return lax.ppermute(value, "cp", x_route(1)), lax.ppermute(value, "cp", x_route(-1))


def x_far(near):
    below, above = near
    half = (below.shape[0] // 2 + 15) // 16 * 16
    return lax.ppermute(below[:half], "cp", x_route(1)), lax.ppermute(above[half:], "cp", x_route(-1))


def section(queries, keys, values, out_weight, span_order):
    n_pp = lax.axis_size("pp")
    span = queries.shape[1] // 2
    pp, cp, tp = (lax.axis_index(a) for a in ("pp", "cp", "tp"))
    zr = (cp // SIDE) ^ jnp.where(pp % SIDE == 0, SHIFT, 0)
    x = cp % SIDE
    swap = [(0, 1), (1, 0)]

    kv = jnp.concatenate([keys[0], values[0]], axis=1)
    kv = lax.ppermute(kv, ("pp", "cp"), section_route(n_pp))
    slots = [kv] + [lax.ppermute(kv, "cp", z_route(k)) for k in range(1, SIDE)]
    qa = lax.ppermute(queries[0, :span], ("pp", "cp"), section_route(n_pp))
    qy = lax.ppermute(queries[0, span:], "pp", y_route(n_pp))
    qg = lax.ppermute(qy, ("pp", "cp"), gap_route(n_pp))
    qs = (qa, jnp.where(pp % SIDE == 0, qg, qy))
    weights = lax.ppermute(out_weight, "tp", swap)
    weights = (out_weight, hold(weights))
    kv = jnp.concatenate(slots, axis=0)
    kv_all = (kv, *x_near(kv), lax.ppermute(kv, "cp", x_route(2)))

    here = jnp.stack([zr, x, tp]).astype(jnp.int32)
    kept, given = attend(here, span_order, qs, kv_all, span)
    taken = lax.ppermute(given, "tp", swap)
    mine = jnp.concatenate([kept, taken], axis=1)

    half = span // 2
    near0 = x_near(mine)
    z2_parts = lax.ppermute(kept, "cp", z_route(2)), lax.ppermute(taken, "cp", z_route(2))
    z2 = jnp.concatenate(z2_parts, axis=1)
    z1 = lax.ppermute(mine[BUNDLED:], "cp", z_route(1))
    far0 = x_far(near0)
    zt = lax.ppermute(mine[:BUNDLED], "cp", z_route(1))
    near1 = x_near(z1)
    tops = jnp.concatenate([near0[0][:BUNDLED], near0[1][:BUNDLED], far0[0], far0[1][: BUNDLED - half]], axis=0)
    b1 = lax.ppermute(tops, "cp", z_route(1))
    far1 = x_far(near1)
    near2 = x_near(z2)
    z3 = lax.ppermute(z2, "cp", z_route(1))
    near3 = x_near(z3)
    far2 = x_far(near2)
    far3 = x_far(near3)

    shape = (lax.axis_size("cp"), span, out_weight.shape[1])
    left, right, far = SIDE - 1, 1, 2

    def near_of(k, pair):
        return [(a, 0, a.shape[0], k, offset, span - a.shape[0]) for a, offset in zip(pair, (left, right))]

    def far_of(k, pair):
        top, bottom = (a.shape[0] for a in pair)
        return [(pair[0], 0, top, k, far, span - top - bottom), (pair[1], 0, bottom, k, far, span - bottom)]

    first = [(mine, 0, span, 0, 0, 0), *near_of(0, near0), *far_of(0, far0)]
    second = [(z2, 0, span, 2, 0, 0), *near_of(2, near2), (z3, 0, span, 3, 0, 0)]
    second += [(zt, 0, BUNDLED, 1, 0, 0), (z1, 0, span - BUNDLED, 1, 0, BUNDLED)]
    second += [*near_of(1, near1), *far_of(1, far1)]
    third = near_of(3, near3)
    third += [(b1, i * BUNDLED, BUNDLED, 1, offset, 0) for i, offset in enumerate((left, right, far))]
    fourth = [*far_of(2, far2), *far_of(3, far3)]
    out = None
    for pieces in (first, second, third, fourth):
        out = project(here, pieces, weights, out, shape)
    return out[None]


def solution(mesh):
    placed = (P("pp", "cp", "tp"), P("pp", "cp", "tp"), P("pp", "cp", "tp"), P("tp", "cp"), P())
    return jax.shard_map(section, mesh=mesh, in_specs=placed, out_specs=P("pp", None, "tp", "cp"), check_vma=False)
```
